32 devices in a mesh: rep: 2 (over x), dp: 16 (over y, z, core).
Axes of the slice: x: 2, y: 2, z: 4, core: 2. Of those that a mesh axis runs over, the one named last changes fastest.
Arguments:
- a: bfloat16 [32, 4, 8192, 1024], P(('rep', 'dp')), parts along dimension 0
- g: bfloat16 [32, 4, 8192, 2816], P(('rep', 'dp')), parts along dimension 0
Outputs:
- output: bfloat16 [8, 1024, 2816], P('rep'), parts along dimension 0
There are 2 independent parts. The reference program is written for one: setup_inputs(seed, part) draws one part's arguments, and reference() takes and returns one part's arrays. A program takes and returns all parts, laid end to end along the dimension named above; each array names one.
All inputs are finite; a program needn't handle non-finite values.
Results may differ from the reference program's by a relative error of at most 0.012.
Values are sent between devices in bfloat16 or wider.
A program may use at most 2 GiB of HBM per device.

```python
import jax
import jax.numpy as jnp
from jax import lax

DEVICES = 16
MATRICES = 4
TOKENS = 8192
D = 1024
FF = 2816


def setup_inputs(seed: int = 0, part: int = 0) -> dict:
    ka, kg, ks = (jax.random.fold_in(k, part) for k in jax.random.split(jax.random.key(seed), 3))
    size = 2.0 ** jax.random.uniform(ks, (DEVICES, MATRICES, 1, 1), jnp.float32, -1.0, 1.0)
    a = jax.random.normal(ka, (DEVICES, MATRICES, TOKENS, D), jnp.float32)
    g = size * jax.random.normal(kg, (DEVICES, MATRICES, TOKENS, FF), jnp.float32) * (DEVICES * TOKENS) ** -0.5
    return {"a": a.astype(jnp.bfloat16), "g": g.astype(jnp.bfloat16)}


def reference(a, g):
    def take(so_far, one):
        return so_far + jnp.einsum("ntd,ntf->ndf", *one, preferred_element_type=jnp.float32), None

    return lax.scan(take, jnp.zeros((MATRICES, D, FF), jnp.float32), (a, g))[0].astype(jnp.bfloat16)
```

```python
import functools

import jax
import jax.numpy as jnp
from jax import lax
from jax.experimental import pallas as pl
from jax.experimental.pallas import tpu as pltpu
from jax.sharding import PartitionSpec as P

CW = 256
LAG = (1, 3, 5, 7, 9, 11, 13, 15)
WL = 16
WS = 8
WF = 4
VMEM_LIMIT = 67043328
F32, BF16 = jnp.float32, jnp.bfloat16


def kernel(a, g, out, av, gv, acc, s0s, s0r, sbuf, ra, rb, rc, fbuf,
           a_sem, g_sem, s0_ssem, s0_rsem, r_ssem, ra_sem, rb_sem, rc_sem, b_ssem, b_rsem, p_rsem):
    matrices, tokens, depth = a.shape
    per = g.shape[2] // CW
    blocks = matrices * per
    q = depth // 8
    half, quarter = 4 * q, 2 * q

    me = lax.axis_index("dp")
    core, z, y = me % 2, (me // 2) % 4, me // 8
    zi = z // 2
    mid = jnp.logical_or(z == 1, z == 2)
    end = jnp.logical_not(mid)
    yf, zf = core == 0, core == 1
    partner = me + 1 - 2 * core
    across = me + 8 - 16 * y
    side = me + 2 - 4 * (z % 2)
    other = me + 2 * (3 - 2 * z)

    def both(*conditions):
        return functools.reduce(jnp.logical_and, conditions)

    def rows(start, size):
        return pl.ds(pl.multiple_of(start, q), size)

    def piece(r, zz):
        return core * half + r * (quarter - q * core) + zz * (q + q * core)

    def place(j, start, size=q):
        columns = pl.ds(pl.multiple_of((j % per) * CW, CW), CW)
        return out.at[j // per, rows(start, size), columns]

    def remote(src, dst, ssem, rsem, to):
        return pltpu.make_async_remote_copy(
            src_ref=src, dst_ref=dst, send_sem=ssem, recv_sem=rsem,
            device_id={"dp": to}, device_id_type=pl.DeviceIdType.MESH)

    def a_load(n):
        return pltpu.make_async_copy(a.at[n], av.at[n % 2], a_sem.at[n % 2])

    def g_load(i):
        columns = pl.ds(pl.multiple_of((i % per) * CW, CW), CW)
        return pltpu.make_async_copy(g.at[i // per, :, columns], gv.at[i % 2], g_sem.at[i % 2])

    def s0(i):
        return remote(s0s.at[i % WF], s0r.at[i % WF], s0_ssem.at[i % WF], s0_rsem.at[i % WF], partner)

    def to_a(j, start, size, to, k):
        return remote(sbuf.at[j % WS, rows(start, size)], ra.at[j % WL, pl.ds(0, size)],
                      r_ssem.at[k, j % WF], ra_sem.at[j % WL], to)

    def to_b(j, start, to, k):
        return remote(sbuf.at[j % WS, rows(start, quarter)], rb.at[j % WS],
                      r_ssem.at[k, j % WF], rb_sem.at[j % WS], to)

    def to_c(j, start, to):
        return remote(sbuf.at[j % WS, rows(start, q)], rc.at[j % WS],
                      r_ssem.at[2, j % WF], rc_sem.at[j % WS], to)

    def finished(j, r, zz, slot, kind, to, src=None):
        at = place(j, piece(r, zz))
        return remote(at if src is None else src, at, b_ssem.at[slot, j % WF], b_rsem.at[kind, j % WL], to)

    def beside(j, r, zz, slot, src=None):
        at = place(j, piece(r, zz))
        return remote(at if src is None else src, at, b_ssem.at[slot, j % WF], p_rsem.at[r * 2 + zz, j % WL], partner)

    def arrived(j, r, zz, kind):
        finished(j, r, zz, 0, kind, partner).wait_recv()

    def sent(j, *slots):
        for slot in slots:
            finished(j, 0, 0, slot, 0, partner).wait_send()

    def mine(j, start, size):
        return acc.at[j % WS, rows(core * half + start, size)]

    def plus(x, y):
        return x[...] + y[...].astype(F32)

    def multiply(i):
        g_load(i).wait()

        @pl.when(i % per == 0)
        def _():
            a_load(i // per).wait()

        @pl.when(both(i % per == 0, i // per + 1 < matrices))
        def _():
            a_load(i // per + 1).start()

        acc[i % WS] = lax.dot_general(av[(i // per) % 2], gv[i % 2], (((0,), (0,)), ((), ())),
                                      preferred_element_type=F32)
        s0s[i % WF] = acc[i % WS, rows((1 - core) * half, half)].astype(BF16)

        @pl.when(i + 2 < blocks)
        def _():
            g_load(i + 2).start()

        s0(i).start()

    def stage1(j):
        s0(j).wait()
        theirs = s0r.at[j % WF]

        @pl.when(yf)
        def _():
            away, own = (1 - y) * quarter, y * quarter
            sbuf[j % WS, rows(away, quarter)] = plus(mine(j, away, quarter), theirs.at[rows(away, quarter)]).astype(BF16)
            to_b(j, away, across, 0).start()
            mine(j, own, quarter)[...] = plus(mine(j, own, quarter), theirs.at[rows(own, quarter)])

        @pl.when(both(zf, end))
        def _():
            sbuf[j % WS] = plus(mine(j, 0, half), theirs).astype(BF16)
            to_a(j, 0, half, side, 0).start()

        @pl.when(both(zf, mid))
        def _():
            mine(j, 0, half)[...] = plus(mine(j, 0, half), theirs)

    def stage2(j):
        @pl.when(yf)
        def _():
            own = y * quarter
            to_b(j, (1 - y) * quarter, across, 0).wait()

            @pl.when(end)
            def _():
                sbuf[j % WS, rows(own, quarter)] = plus(mine(j, own, quarter), rb.at[j % WS]).astype(BF16)
                to_a(j, own, quarter, side, 1).start()

            @pl.when(mid)
            def _():
                mine(j, own, quarter)[...] = plus(mine(j, own, quarter), rb.at[j % WS])

        @pl.when(both(zf, end))
        def _():
            to_a(j, 0, half, side, 0).wait_send()

        @pl.when(both(zf, mid))
        def _():
            to_a(j, 0, half, side, 0).wait_recv()
            away, own = (1 - zi) * quarter, zi * quarter
            theirs = ra.at[j % WL]
            sbuf[j % WS, rows(away, quarter)] = plus(mine(j, away, quarter), theirs.at[rows(away, quarter)]).astype(BF16)
            to_b(j, away, other, 1).start()
            mine(j, own, quarter)[...] = plus(mine(j, own, quarter), theirs.at[rows(own, quarter)])

    def stage3(j):
        @pl.when(both(yf, end))
        def _():
            to_a(j, y * quarter, quarter, side, 1).wait_send()

        @pl.when(both(yf, mid))
        def _():
            to_a(j, y * quarter, quarter, side, 1).wait_recv()
            away, own = (1 - zi) * q, zi * q
            theirs = ra.at[j % WL]
            sbuf[j % WS, rows(y * quarter + away, q)] = plus(
                mine(j, y * quarter + away, q), theirs.at[rows(away, q)]).astype(BF16)
            to_c(j, y * quarter + away, other).start()
            mine(j, y * quarter + own, q)[...] = plus(mine(j, y * quarter + own, q), theirs.at[rows(own, q)])

        @pl.when(both(zf, mid))
        def _():
            to_b(j, (1 - zi) * quarter, other, 1).wait()
            away, own = (1 - y) * q, y * q
            theirs = rb.at[j % WS]
            sbuf[j % WS, rows(zi * quarter + away, q)] = plus(
                mine(j, zi * quarter + away, q), theirs.at[rows(away, q)]).astype(BF16)
            to_c(j, zi * quarter + away, across).start()
            mine(j, zi * quarter + own, q)[...] = plus(mine(j, zi * quarter + own, q), theirs.at[rows(own, q)])

    def stage4(j):
        @pl.when(mid)
        def _():
            to_c(j, 0, partner).wait()
            f = fbuf.at[j % WF]
            f[...] = plus(acc.at[j % WS, rows(piece(y, zi), q)], rc.at[j % WS]).astype(BF16)
            finished(j, y, zi, 0, 0, other, f).start()
            finished(j, y, zi, 1, 1, across, f).start()
            finished(j, y, zi, 2, 0, side, f).start()
            beside(j, y, zi, 3, f).start()
            pltpu.make_async_copy(f, place(j, piece(y, zi)), b_ssem.at[4, j % WF]).start()

    def stage5(j):
        @pl.when(mid)
        def _():
            sent(j, 0, 1, 2, 3)
            pltpu.make_async_copy(fbuf.at[j % WF], place(j, piece(y, zi)), b_ssem.at[4, j % WF]).wait()
            arrived(j, y, 1 - zi, 0)

            @pl.when(yf)
            def _():
                finished(j, y, 1 - zi, 5, 1, side).start()
                finished(j, y, 1 - zi, 6, 2, across).start()

            @pl.when(zf)
            def _():
                finished(j, y, 1 - zi, 5, 2, side).start()

            beside(j, y, 1 - zi, 7).start()
            arrived(j, 1 - y, zi, 1)

            @pl.when(zf)
            def _():
                finished(j, 1 - y, zi, 6, 2, other).start()
                finished(j, 1 - y, zi, 9, 1, side).start()

            beside(j, 1 - y, zi, 8).start()

        @pl.when(end)
        def _():
            arrived(j, y, zi, 0)

            @pl.when(yf)
            def _():
                finished(j, y, zi, 6, 2, across).start()

            beside(j, y, zi, 5).start()

    def stage6(j):
        @pl.when(mid)
        def _():
            sent(j, 5, 6, 7, 8)

            @pl.when(zf)
            def _():
                sent(j, 9)

            arrived(j, 1 - y, 1 - zi, 2)

            @pl.when(zf)
            def _():
                finished(j, 1 - y, 1 - zi, 11, 3, side).start()

            beside(j, 1 - y, 1 - zi, 10).start()

        @pl.when(end)
        def _():
            sent(j, 5)

        @pl.when(both(end, yf))
        def _():
            sent(j, 6)
            arrived(j, y, 1 - zi, 1)
            finished(j, y, 1 - zi, 11, 3, across).start()
            beside(j, y, 1 - zi, 10).start()
            arrived(j, 1 - y, zi, 2)
            beside(j, 1 - y, zi, 12).start()

        @pl.when(both(end, zf))
        def _():
            arrived(j, 1 - y, zi, 1)
            beside(j, 1 - y, zi, 10).start()
            arrived(j, y, 1 - zi, 2)
            beside(j, y, 1 - zi, 12).start()

    def stage7(j):
        sent(j, 10)

        @pl.when(both(zf, mid))
        def _():
            sent(j, 11)

        @pl.when(both(yf, end))
        def _():
            sent(j, 11)

        @pl.when(end)
        def _():
            sent(j, 12)
            arrived(j, 1 - y, 1 - zi, 3)
            beside(j, 1 - y, 1 - zi, 13).start()

    def stage8(j):
        @pl.when(end)
        def _():
            sent(j, 13)

        for k in range(4):
            beside(j, k // 2, k % 2, 0).wait_recv()

    a_load(0).start()
    g_load(0).start()
    g_load(1).start()

    barrier = pltpu.get_barrier_semaphore()

    def hello(to):
        pl.semaphore_signal(barrier, inc=1, device_id={"dp": to}, device_id_type=pl.DeviceIdType.MESH)

    for to in (partner, across, side):
        hello(to)

    @pl.when(mid)
    def _():
        hello(other)
        pl.semaphore_wait(barrier, 4)

    @pl.when(end)
    def _():
        pl.semaphore_wait(barrier, 3)

    stages = (stage1, stage2, stage3, stage4, stage5, stage6, stage7, stage8)

    def tick(i, carry):
        @pl.when(i < blocks)
        def _():
            multiply(i)

        for stage, lag in zip(stages, LAG):
            pl.when(both(i >= lag, i < blocks + lag))(functools.partial(stage, i - lag))
        return carry

    lax.fori_loop(0, blocks + LAG[-1], tick, 0)


def solution(mesh):
    def step(a, g):
        _, matrices, tokens, depth = a.shape
        width = g.shape[3]
        q = depth // 8
        dma = pltpu.SemaphoreType.DMA
        return pl.pallas_call(
            kernel,
            out_shape=jax.ShapeDtypeStruct((matrices, depth, width), BF16),
            in_specs=[pl.BlockSpec(memory_space=pl.ANY)] * 2,
            out_specs=pl.BlockSpec(memory_space=pl.ANY),
            scratch_shapes=[
                pltpu.VMEM((2, tokens, depth), BF16),
                pltpu.VMEM((2, tokens, CW), BF16),
                pltpu.VMEM((WS, depth, CW), F32),
                pltpu.VMEM((WF, 4 * q, CW), BF16),
                pltpu.VMEM((WF, 4 * q, CW), BF16),
                pltpu.VMEM((WS, 4 * q, CW), BF16),
                pltpu.VMEM((WL, 4 * q, CW), BF16),
                pltpu.VMEM((WS, 2 * q, CW), BF16),
                pltpu.VMEM((WS, q, CW), BF16),
                pltpu.VMEM((WF, q, CW), BF16),
                dma((2,)), dma((2,)), dma((WF,)), dma((WF,)), dma((3, WF)), dma((WL,)), dma((WS,)), dma((WS,)),
                dma((14, WF)), dma((4, WL)), dma((4, WL)),
            ],
            compiler_params=pltpu.CompilerParams(
                collective_id=0, has_side_effects=True, vmem_limit_bytes=VMEM_LIMIT),
            cost_estimate=pl.CostEstimate(
                flops=2 * matrices * tokens * depth * width,
                bytes_accessed=2 * matrices * (tokens * (depth + width) + depth * width), transcendentals=0),
            name="sums",
        )(a[0], g[0])

    return jax.shard_map(
        step, mesh=mesh,
        in_specs=(P(("rep", "dp"), None, None, None),) * 2,
        out_specs=P("rep", None, None), check_vma=False)
```

```python
import functools

import jax
import jax.numpy as jnp
from jax import lax
from jax.experimental import pallas as pl
from jax.experimental.pallas import tpu as pltpu
from jax.sharding import PartitionSpec as P

CW = 256
LAG = (1, 2, 3, 4, 5, 7, 9, 10)
WL = 16
WS = 8
WF = 4
VMEM_LIMIT = 67043328
F32, BF16 = jnp.float32, jnp.bfloat16


PARTS = 8


def kernel(a, g, out, av, gv, acc, s0r, sbuf, ra, rb, rc, fbuf,
           a_sem, g_sem, first_sem, s0_ssem, s0_rsem, r_ssem, ra_sem, rb_sem, rc_sem, b_ssem, b_rsem, p_rsem):
    matrices, tokens, depth = a.shape
    per = g.shape[2] // CW
    blocks = matrices * per
    q = depth // 8
    half, quarter = 4 * q, 2 * q

    me = lax.axis_index("dp")
    core, z, y = me % 2, (me // 2) % 4, me // 8
    zi = z // 2
    mid = jnp.logical_or(z == 1, z == 2)
    end = jnp.logical_not(mid)
    yf, zf = core == 0, core == 1
    partner = me + 1 - 2 * core
    across = me + 8 - 16 * y
    side = me + 2 - 4 * (z % 2)
    other = me + 2 * (3 - 2 * z)

    def both(*conditions):
        return functools.reduce(jnp.logical_and, conditions)

    def rows(start, size):
        return pl.ds(pl.multiple_of(start, q), size)

    def piece(r, zz):
        return core * half + r * (quarter - q * core) + zz * (q + q * core)

    def place(j, start, size=q):
        columns = pl.ds(pl.multiple_of((j % per) * CW, CW), CW)
        return out.at[j // per, rows(start, size), columns]

    def remote(src, dst, ssem, rsem, to):
        return pltpu.make_async_remote_copy(
            src_ref=src, dst_ref=dst, send_sem=ssem, recv_sem=rsem,
            device_id={"dp": to}, device_id_type=pl.DeviceIdType.MESH)

    def a_load(n):
        return pltpu.make_async_copy(a.at[n], av.at[n % 2], a_sem.at[n % 2])

    def g_load(i):
        columns = pl.ds(pl.multiple_of((i % per) * CW, CW), CW)
        return pltpu.make_async_copy(g.at[i // per, :, columns], gv.at[i % 2], g_sem.at[i % 2])

    def s0(i):
        return remote(acc.at[i % WS, rows((1 - core) * half, half)], s0r.at[i % WF], s0_ssem.at[i % WF], s0_rsem.at[i % WF], partner)

    def to_a(j, start, size, to, k):
        return remote(sbuf.at[j % WS, rows(start, size)], ra.at[j % WL, pl.ds(0, size)],
                      r_ssem.at[k, j % WF], ra_sem.at[j % WL], to)

    def to_b(j, start, to, k):
        return remote(sbuf.at[j % WS, rows(start, quarter)], rb.at[j % WS],
                      r_ssem.at[k, j % WF], rb_sem.at[j % WS], to)

    def to_c(j, start, to):
        return remote(sbuf.at[j % WS, rows(start, q)], rc.at[j % WS],
                      r_ssem.at[2, j % WF], rc_sem.at[j % WS], to)

    def finished(j, start, size, slot, kind, to, src=None):
        at = place(j, start, size)
        return remote(at if src is None else src, at, b_ssem.at[slot, j % WF], b_rsem.at[kind, j % WL], to)

    def beside(j, which):
        at = place(j, which * half, half)
        return remote(at, at, b_ssem.at[7, j % WF], p_rsem.at[j % WL], partner)

    def kept(j):
        return pltpu.make_async_copy(fbuf.at[j % WF], place(j, piece(y, zi)), b_ssem.at[4, j % WF])

    def mine(j, start, size):
        return acc.at[j % WS, rows(core * half + start, size)]

    def plus(x, y):
        return x[...] + y[...].astype(F32)

    def first_loads(k):
        depths = pl.ds(k * (tokens // PARTS), tokens // PARTS)
        return (pltpu.make_async_copy(a.at[0, depths], av.at[0, depths], first_sem.at[0, k]),
                pltpu.make_async_copy(g.at[0, depths, pl.ds(0, CW)], gv.at[0, depths], first_sem.at[1, k]))

    def product(x, w):
        return lax.dot_general(x, w, (((0,), (0,)), ((), ())), preferred_element_type=F32)

    def multiply(i):
        @pl.when(i == 0)
        def _():
            acc[0] = jnp.zeros(acc.shape[1:], F32)

            def part(k, carry):
                for load in first_loads(k):
                    load.wait()
                depths = pl.ds(k * (tokens // PARTS), tokens // PARTS)
                acc[0] += product(av[0, depths], gv[0, depths])
                return carry

            lax.fori_loop(0, PARTS, part, 0)

        @pl.when(i > 0)
        def _():
            g_load(i).wait()

            @pl.when(i % per == 0)
            def _():
                a_load(i // per).wait()

            @pl.when(both(i % per == 1, i // per + 1 < matrices))
            def _():
                a_load(i // per + 1).start()

            acc[i % WS] = product(av[(i // per) % 2], gv[i % 2])

        @pl.when(i + 2 < blocks)
        def _():
            g_load(i + 2).start()

        s0(i).start()

    def stage1(j):
        s0(j).wait()
        theirs = s0r.at[j % WF]

        @pl.when(yf)
        def _():
            away, own = (1 - y) * quarter, y * quarter
            sbuf[j % WS, rows(away, quarter)] = plus(mine(j, away, quarter), theirs.at[rows(away, quarter)]).astype(BF16)
            to_b(j, away, across, 0).start()
            mine(j, own, quarter)[...] = plus(mine(j, own, quarter), theirs.at[rows(own, quarter)])

        @pl.when(both(zf, end))
        def _():
            sbuf[j % WS] = plus(mine(j, 0, half), theirs).astype(BF16)
            to_a(j, 0, half, side, 0).start()

        @pl.when(both(zf, mid))
        def _():
            mine(j, 0, half)[...] = plus(mine(j, 0, half), theirs)

    def stage2(j):
        @pl.when(yf)
        def _():
            own = y * quarter
            to_b(j, (1 - y) * quarter, across, 0).wait()

            @pl.when(end)
            def _():
                sbuf[j % WS, rows(own, quarter)] = plus(mine(j, own, quarter), rb.at[j % WS]).astype(BF16)
                to_a(j, own, quarter, side, 1).start()

            @pl.when(mid)
            def _():
                mine(j, own, quarter)[...] = plus(mine(j, own, quarter), rb.at[j % WS])

        @pl.when(both(zf, end))
        def _():
            to_a(j, 0, half, side, 0).wait_send()

        @pl.when(both(zf, mid))
        def _():
            to_a(j, 0, half, side, 0).wait_recv()
            away, own = (1 - zi) * quarter, zi * quarter
            theirs = ra.at[j % WL]
            sbuf[j % WS, rows(away, quarter)] = plus(mine(j, away, quarter), theirs.at[rows(away, quarter)]).astype(BF16)
            to_b(j, away, other, 1).start()
            mine(j, own, quarter)[...] = plus(mine(j, own, quarter), theirs.at[rows(own, quarter)])

    def stage3(j):
        @pl.when(both(yf, end))
        def _():
            to_a(j, y * quarter, quarter, side, 1).wait_send()

        @pl.when(both(yf, mid))
        def _():
            to_a(j, y * quarter, quarter, side, 1).wait_recv()
            away, own = (1 - zi) * q, zi * q
            theirs = ra.at[j % WL]
            sbuf[j % WS, rows(y * quarter + away, q)] = plus(
                mine(j, y * quarter + away, q), theirs.at[rows(away, q)]).astype(BF16)
            to_c(j, y * quarter + away, other).start()
            mine(j, y * quarter + own, q)[...] = plus(mine(j, y * quarter + own, q), theirs.at[rows(own, q)])

        @pl.when(both(zf, mid))
        def _():
            to_b(j, (1 - zi) * quarter, other, 1).wait()
            away, own = (1 - y) * q, y * q
            theirs = rb.at[j % WS]
            sbuf[j % WS, rows(zi * quarter + away, q)] = plus(
                mine(j, zi * quarter + away, q), theirs.at[rows(away, q)]).astype(BF16)
            to_c(j, zi * quarter + away, across).start()
            mine(j, zi * quarter + own, q)[...] = plus(mine(j, zi * quarter + own, q), theirs.at[rows(own, q)])

    def stage4(j):
        @pl.when(mid)
        def _():
            to_c(j, 0, partner).wait()
            f = fbuf.at[j % WF]
            f[...] = plus(acc.at[j % WS, rows(piece(y, zi), q)], rc.at[j % WS]).astype(BF16)

            @pl.when(yf)
            def _():
                finished(j, piece(y, zi), q, 0, 0, other, f).start()

            @pl.when(zf)
            def _():
                finished(j, piece(y, zi), q, 0, 0, across, f).start()
                finished(j, piece(y, zi), q, 1, 1, other, f).start()
                finished(j, piece(y, zi), q, 2, 0, side, f).start()

            kept(j).start()

    def stage5(j):
        @pl.when(mid)
        def _():
            kept(j).wait()
            finished(j, 0, q, 0, 0, partner).wait()

        @pl.when(both(yf, mid))
        def _():
            finished(j, y * quarter, quarter, 5, 0, side).start()
            finished(j, y * quarter, quarter, 6, 1, across).start()

        @pl.when(both(zf, mid))
        def _():
            finished(j, piece(1 - y, zi), q, 5, 2, other).start()
            finished(j, 0, q, 1, 1, partner).wait()
            finished(j, piece(y, 1 - zi), q, 6, 1, side).start()
            finished(j, 0, q, 2, 0, partner).wait_send()

        @pl.when(both(zf, end))
        def _():
            finished(j, 0, q, 0, 0, partner).wait_recv()
            finished(j, piece(y, zi), q, 5, 2, across).start()

    def stage6(j):
        @pl.when(both(yf, mid))
        def _():
            finished(j, 0, quarter, 5, 1, partner).wait()
            finished(j, 0, quarter, 6, 1, partner).wait_send()

        @pl.when(both(zf, mid))
        def _():
            finished(j, 0, q, 5, 2, partner).wait()
            finished(j, 0, q, 6, 2, partner).wait_send()

        @pl.when(mid)
        def _():
            beside(j, core).start()

        @pl.when(both(yf, end))
        def _():
            finished(j, 0, quarter, 6, 0, partner).wait_recv()
            finished(j, y * quarter, quarter, 6, 1, across).start()

        @pl.when(both(zf, end))
        def _():
            finished(j, 0, q, 5, 1, partner).wait()
            finished(j, piece(y, 1 - zi), q, 6, 3, across).start()

    def stage7(j):
        @pl.when(both(yf, end))
        def _():
            finished(j, 0, quarter, 6, 1, partner).wait()

        @pl.when(both(zf, end))
        def _():
            finished(j, 0, q, 6, 2, partner).wait()
            finished(j, 0, q, 6, 3, partner).wait_recv()

        @pl.when(end)
        def _():
            beside(j, core).start()

    def stage8(j):
        beside(j, 1 - core).wait()

    for k in range(PARTS):
        for load in first_loads(k):
            load.start()
    g_load(1).start()

    barrier = pltpu.get_barrier_semaphore()

    def hello(to):
        pl.semaphore_signal(barrier, inc=1, device_id={"dp": to}, device_id_type=pl.DeviceIdType.MESH)

    for to in (partner, across, side):
        hello(to)

    @pl.when(mid)
    def _():
        hello(other)
        pl.semaphore_wait(barrier, 4)

    @pl.when(end)
    def _():
        pl.semaphore_wait(barrier, 3)

    stages = (stage1, stage2, stage3, stage4, stage5, stage6, stage7, stage8)

    def tick(i, carry):
        @pl.when(i < blocks)
        def _():
            multiply(i)

        for stage, lag in zip(stages, LAG):
            pl.when(both(i >= lag, i < blocks + lag))(functools.partial(stage, i - lag))
        return carry

    lax.fori_loop(0, blocks + LAG[-1], tick, 0)


def place_kernel(x, o, held, in_sem, out_sem):
    matrices, bands, size, _ = held.shape
    every = [(n, b) for n in range(matrices) for b in range(bands)]

    def load(n, b):
        return pltpu.make_async_copy(x.at[n, pl.ds(b * size, size)], held.at[n, b], in_sem.at[n, b])

    def store(n, b):
        return pltpu.make_async_copy(held.at[n, b], o.at[n, pl.ds(b * size, size)], out_sem.at[n, b])

    for nb in every:
        load(*nb).start()
    for nb in every:
        load(*nb).wait()
        store(*nb).start()
    for nb in every:
        store(*nb).wait()


def solution(mesh):
    def step(a, g):
        _, matrices, tokens, depth = a.shape
        width = g.shape[3]
        q = depth // 8
        dma = pltpu.SemaphoreType.DMA
        sums = pl.pallas_call(
            kernel,
            out_shape=jax.ShapeDtypeStruct((matrices, depth, width), BF16),
            in_specs=[pl.BlockSpec(memory_space=pl.ANY)] * 2,
            out_specs=pl.BlockSpec(memory_space=pl.ANY),
            scratch_shapes=[
                pltpu.VMEM((2, tokens, depth), BF16),
                pltpu.VMEM((2, tokens, CW), BF16),
                pltpu.VMEM((WS, depth, CW), F32),
                pltpu.VMEM((WF, 4 * q, CW), F32),
                pltpu.VMEM((WS, 4 * q, CW), BF16),
                pltpu.VMEM((WL, 4 * q, CW), BF16),
                pltpu.VMEM((WS, 2 * q, CW), BF16),
                pltpu.VMEM((WS, q, CW), BF16),
                pltpu.VMEM((WF, q, CW), BF16),
                dma((2,)), dma((2,)), dma((2, PARTS)), dma((WF,)), dma((WF,)), dma((3, WF)), dma((WL,)), dma((WS,)), dma((WS,)),
                dma((8, WF)), dma((4, WL)), dma((WL,)),
            ],
            compiler_params=pltpu.CompilerParams(
                collective_id=0, has_side_effects=True, vmem_limit_bytes=VMEM_LIMIT),
            cost_estimate=pl.CostEstimate(
                flops=2 * matrices * tokens * depth * width,
                bytes_accessed=2 * matrices * (tokens * (depth + width) + depth * width), transcendentals=0),
            name="sums",
        )(a[0], g[0])
        bands = (matrices, 4, depth // 4, width)
        return pl.pallas_call(
            place_kernel,
            out_shape=jax.ShapeDtypeStruct(sums.shape, BF16),
            in_specs=[pl.BlockSpec(memory_space=pl.ANY)],
            out_specs=pl.BlockSpec(memory_space=pl.ANY),
            scratch_shapes=[pltpu.VMEM(bands, BF16), dma(bands[:2]), dma(bands[:2])],
            compiler_params=pltpu.CompilerParams(vmem_limit_bytes=VMEM_LIMIT),
            cost_estimate=pl.CostEstimate(flops=0, bytes_accessed=4 * matrices * depth * width, transcendentals=0),
            name="place",
        )(sums)

    return jax.shard_map(
        step, mesh=mesh,
        in_specs=(P(("rep", "dp"), None, None, None),) * 2,
        out_specs=P("rep", None, None), check_vma=False)
```

```python
import functools

import jax
import jax.numpy as jnp
from jax import lax
from jax.experimental import pallas as pl
from jax.experimental.pallas import tpu as pltpu
from jax.sharding import PartitionSpec as P

CW = 256
LAG = (1, 2, 3, 4, 5, 7, 9, 10)
WL = 12
WS = 8
WA = 6
WF = 4
VMEM_LIMIT = 67043328
F32, BF16 = jnp.float32, jnp.bfloat16


PARTS = 8


def kernel(a, g, out, av, gv, acc, s0r, sbuf, ra, rb, rc, fin,
           a_sem, g_sem, first_sem, s0_ssem, s0_rsem, r_ssem, ra_sem, rb_sem, rc_sem, b_ssem, b_rsem, p_rsem):
    matrices, tokens, depth = a.shape
    per = g.shape[2] // CW
    blocks = matrices * per
    q = depth // 8
    half, quarter = 4 * q, 2 * q

    me = lax.axis_index("dp")
    core, z, y = me % 2, (me // 2) % 4, me // 8
    zi = z // 2
    mid = jnp.logical_or(z == 1, z == 2)
    end = jnp.logical_not(mid)
    yf, zf = core == 0, core == 1
    partner = me + 1 - 2 * core
    across = me + 8 - 16 * y
    side = me + 2 - 4 * (z % 2)
    other = me + 2 * (3 - 2 * z)

    def both(*conditions):
        return functools.reduce(jnp.logical_and, conditions)

    def rows(start, size):
        return pl.ds(pl.multiple_of(start, q), size)

    def piece(r, zz):
        return r * (quarter - q * core) + zz * (q + q * core)

    def place(j, start, size=q):
        columns = pl.ds(pl.multiple_of((j % per) * CW, CW), CW)
        return out.at[j // per, rows(start, size), columns]

    def remote(src, dst, ssem, rsem, to):
        return pltpu.make_async_remote_copy(
            src_ref=src, dst_ref=dst, send_sem=ssem, recv_sem=rsem,
            device_id={"dp": to}, device_id_type=pl.DeviceIdType.MESH)

    def a_load(n):
        return pltpu.make_async_copy(a.at[n], av.at[n % 2], a_sem.at[n % 2])

    def g_load(i):
        columns = pl.ds(pl.multiple_of((i % per) * CW, CW), CW)
        return pltpu.make_async_copy(g.at[i // per, :, columns], gv.at[i % 2], g_sem.at[i % 2])

    def s0(i):
        return remote(acc.at[i % WA, rows((1 - core) * half, half)], s0r.at[i % WA], s0_ssem.at[i % WA], s0_rsem.at[i % WA], partner)

    def to_a(j, start, size, to, k):
        return remote(sbuf.at[j % WA, rows(start, size)], ra.at[j % WL, pl.ds(0, size)],
                      r_ssem.at[k, j % WF], ra_sem.at[j % WL], to)

    def to_b(j, start, to, k):
        return remote(sbuf.at[j % WA, rows(start, quarter)], rb.at[j % WS],
                      r_ssem.at[k, j % WF], rb_sem.at[j % WS], to)

    def to_c(j, start, to):
        return remote(sbuf.at[j % WA, rows(start, q)], rc.at[j % WS],
                      r_ssem.at[2, j % WF], rc_sem.at[j % WS], to)

    def finished(j, start, size, slot, kind, to):
        at = fin.at[j % WL, rows(start, size)]
        return remote(at, at, b_ssem.at[slot, j % WF], b_rsem.at[kind, j % WL], to)

    def beside(j, which):
        return remote(fin.at[j % WL], place(j, which * half, half), b_ssem.at[7, j % WF], p_rsem.at[j % WL], partner)

    def kept(j):
        return pltpu.make_async_copy(fin.at[j % WL], place(j, core * half, half), b_ssem.at[4, j % WF])

    def mine(j, start, size):
        return acc.at[j % WA, rows(core * half + start, size)]

    def plus(x, *others):
        return functools.reduce(lambda total, y: total + y[...].astype(F32), others, x[...])

    def beside_sum(j, start, size):
        return s0r.at[j % WA, rows(start, size)]

    def first_loads(k):
        depths = pl.ds(k * (tokens // PARTS), tokens // PARTS)
        return (pltpu.make_async_copy(a.at[0, depths], av.at[0, depths], first_sem.at[0, k]),
                pltpu.make_async_copy(g.at[0, depths, pl.ds(0, CW)], gv.at[0, depths], first_sem.at[1, k]))

    def product(x, w):
        return lax.dot_general(x, w, (((0,), (0,)), ((), ())), preferred_element_type=F32)

    def multiply_first():
        acc[0] = jnp.zeros(acc.shape[1:], F32)

        def part(k, carry):
            for load in first_loads(k):
                load.wait()
            depths = pl.ds(k * (tokens // PARTS), tokens // PARTS)
            acc[0] += product(av[0, depths], gv[0, depths])
            return carry

        lax.fori_loop(0, PARTS, part, 0)
        g_load(2).start()

    def multiply(i):
        g_load(i).wait()

        @pl.when(i % per == 0)
        def _():
            a_load(i // per).wait()

        @pl.when(both(i % per == 1, i // per + 1 < matrices))
        def _():
            a_load(i // per + 1).start()

        acc[i % WA] = product(av[(i // per) % 2], gv[i % 2])

        @pl.when(i + 2 < blocks)
        def _():
            g_load(i + 2).start()

        s0(i).start()

    def stage1(j):
        s0(j).wait()
        theirs = s0r.at[j % WA]

        @pl.when(yf)
        def _():
            away = (1 - y) * quarter
            sbuf[j % WA, rows(away, quarter)] = plus(mine(j, away, quarter), theirs.at[rows(away, quarter)]).astype(BF16)
            to_b(j, away, across, 0).start()

        @pl.when(both(zf, end))
        def _():
            sbuf[j % WA] = plus(mine(j, 0, half), theirs).astype(BF16)
            to_a(j, 0, half, side, 0).start()

    def stage2(j):
        @pl.when(yf)
        def _():
            own = y * quarter
            to_b(j, (1 - y) * quarter, across, 0).wait()

            @pl.when(end)
            def _():
                sbuf[j % WA, rows(own, quarter)] = plus(mine(j, own, quarter), beside_sum(j, own, quarter), rb.at[j % WS]).astype(BF16)
                to_a(j, own, quarter, side, 1).start()

            @pl.when(mid)
            def _():
                mine(j, own, quarter)[...] = plus(mine(j, own, quarter), beside_sum(j, own, quarter), rb.at[j % WS])

        @pl.when(both(zf, end))
        def _():
            to_a(j, 0, half, side, 0).wait_send()

        @pl.when(both(zf, mid))
        def _():
            to_a(j, 0, half, side, 0).wait_recv()
            away, own = (1 - zi) * quarter, zi * quarter
            theirs = ra.at[j % WL]
            sbuf[j % WA, rows(away, quarter)] = plus(
                mine(j, away, quarter), beside_sum(j, away, quarter), theirs.at[rows(away, quarter)]).astype(BF16)
            to_b(j, away, other, 1).start()
            mine(j, own, quarter)[...] = plus(
                mine(j, own, quarter), beside_sum(j, own, quarter), theirs.at[rows(own, quarter)])

    def stage3(j):
        @pl.when(both(yf, end))
        def _():
            to_a(j, y * quarter, quarter, side, 1).wait_send()

        @pl.when(both(yf, mid))
        def _():
            to_a(j, y * quarter, quarter, side, 1).wait_recv()
            away, own = (1 - zi) * q, zi * q
            theirs = ra.at[j % WL]
            sbuf[j % WA, rows(y * quarter + away, q)] = plus(
                mine(j, y * quarter + away, q), theirs.at[rows(away, q)]).astype(BF16)
            to_c(j, y * quarter + away, other).start()
            mine(j, y * quarter + own, q)[...] = plus(mine(j, y * quarter + own, q), theirs.at[rows(own, q)])

        @pl.when(both(zf, mid))
        def _():
            to_b(j, (1 - zi) * quarter, other, 1).wait()
            away, own = (1 - y) * q, y * q
            theirs = rb.at[j % WS]
            sbuf[j % WA, rows(zi * quarter + away, q)] = plus(
                mine(j, zi * quarter + away, q), theirs.at[rows(away, q)]).astype(BF16)
            to_c(j, zi * quarter + away, across).start()
            mine(j, zi * quarter + own, q)[...] = plus(mine(j, zi * quarter + own, q), theirs.at[rows(own, q)])

    def stage4(j):
        @pl.when(mid)
        def _():
            to_c(j, 0, partner).wait()
            fin[j % WL, rows(piece(y, zi), q)] = plus(mine(j, piece(y, zi), q), rc.at[j % WS]).astype(BF16)

            @pl.when(yf)
            def _():
                finished(j, piece(y, zi), q, 0, 0, other).start()

            @pl.when(zf)
            def _():
                finished(j, piece(y, zi), q, 0, 0, across).start()
                finished(j, piece(y, zi), q, 1, 1, other).start()
                finished(j, piece(y, zi), q, 2, 0, side).start()

    def stage5(j):
        @pl.when(mid)
        def _():
            finished(j, 0, q, 0, 0, partner).wait()

        @pl.when(both(yf, mid))
        def _():
            finished(j, y * quarter, quarter, 5, 0, side).start()
            finished(j, y * quarter, quarter, 6, 1, across).start()

        @pl.when(both(zf, mid))
        def _():
            finished(j, piece(1 - y, zi), q, 5, 2, other).start()
            finished(j, 0, q, 1, 1, partner).wait()
            finished(j, piece(y, 1 - zi), q, 6, 1, side).start()
            finished(j, 0, q, 2, 0, partner).wait_send()

        @pl.when(both(zf, end))
        def _():
            finished(j, 0, q, 0, 0, partner).wait_recv()
            finished(j, piece(y, zi), q, 5, 2, across).start()

    def stage6(j):
        @pl.when(both(yf, mid))
        def _():
            finished(j, 0, quarter, 5, 1, partner).wait()
            finished(j, 0, quarter, 6, 1, partner).wait_send()

        @pl.when(both(zf, mid))
        def _():
            finished(j, 0, q, 5, 2, partner).wait()
            finished(j, 0, q, 6, 2, partner).wait_send()

        @pl.when(mid)
        def _():
            beside(j, core).start()
            kept(j).start()

        @pl.when(both(yf, end))
        def _():
            finished(j, 0, quarter, 6, 0, partner).wait_recv()
            finished(j, y * quarter, quarter, 6, 1, across).start()

        @pl.when(both(zf, end))
        def _():
            finished(j, 0, q, 5, 1, partner).wait()
            finished(j, piece(y, 1 - zi), q, 6, 3, across).start()

    def stage7(j):
        @pl.when(both(yf, end))
        def _():
            finished(j, 0, quarter, 6, 1, partner).wait()

        @pl.when(both(zf, end))
        def _():
            finished(j, 0, q, 6, 2, partner).wait()
            finished(j, 0, q, 6, 3, partner).wait_recv()

        @pl.when(end)
        def _():
            beside(j, core).start()
            kept(j).start()

    def stage8(j):
        beside(j, 1 - core).wait()
        kept(j).wait()

    for k in range(PARTS):
        for load in first_loads(k):
            load.start()
    g_load(1).start()

    barrier = pltpu.get_barrier_semaphore()

    def hello(to):
        pl.semaphore_signal(barrier, inc=1, device_id={"dp": to}, device_id_type=pl.DeviceIdType.MESH)

    for to in (partner, across, side):
        hello(to)

    @pl.when(mid)
    def _():
        hello(other)

    multiply_first()

    @pl.when(mid)
    def _():
        pl.semaphore_wait(barrier, 4)

    @pl.when(end)
    def _():
        pl.semaphore_wait(barrier, 3)

    s0(0).start()

    stages = (stage1, stage2, stage3, stage4, stage5, stage6, stage7, stage8)

    def tick(i, carry):
        @pl.when(i < blocks)
        def _():
            multiply(i)

        for stage, lag in zip(stages, LAG):
            pl.when(both(i >= lag, i < blocks + lag))(functools.partial(stage, i - lag))
        return carry

    lax.fori_loop(1, blocks + LAG[-1], tick, 0)


def place_kernel(x, o, held, in_sem, out_sem):
    matrices, bands, size, _ = held.shape
    every = [(n, b) for n in range(matrices) for b in range(bands)]

    def load(n, b):
        return pltpu.make_async_copy(x.at[n, pl.ds(b * size, size)], held.at[n, b], in_sem.at[n, b])

    def store(n, b):
        return pltpu.make_async_copy(held.at[n, b], o.at[n, pl.ds(b * size, size)], out_sem.at[n, b])

    for nb in every:
        load(*nb).start()
    for nb in every:
        load(*nb).wait()
        store(*nb).start()
    for nb in every:
        store(*nb).wait()


def solution(mesh):
    def step(a, g):
        _, matrices, tokens, depth = a.shape
        width = g.shape[3]
        q = depth // 8
        dma = pltpu.SemaphoreType.DMA
        sums = pl.pallas_call(
            kernel,
            out_shape=jax.ShapeDtypeStruct((matrices, depth, width), BF16),
            in_specs=[pl.BlockSpec(memory_space=pl.ANY)] * 2,
            out_specs=pl.BlockSpec(memory_space=pl.ANY),
            scratch_shapes=[
                pltpu.VMEM((2, tokens, depth), BF16),
                pltpu.VMEM((2, tokens, CW), BF16),
                pltpu.VMEM((WA, depth, CW), F32),
                pltpu.VMEM((WA, 4 * q, CW), F32),
                pltpu.VMEM((WA, 4 * q, CW), BF16),
                pltpu.VMEM((WL, 4 * q, CW), BF16),
                pltpu.VMEM((WS, 2 * q, CW), BF16),
                pltpu.VMEM((WS, q, CW), BF16),
                pltpu.VMEM((WL, 4 * q, CW), BF16),
                dma((2,)), dma((2,)), dma((2, PARTS)), dma((WA,)), dma((WA,)), dma((3, WF)), dma((WL,)), dma((WS,)), dma((WS,)),
                dma((8, WF)), dma((4, WL)), dma((WL,)),
            ],
            compiler_params=pltpu.CompilerParams(
                collective_id=0, has_side_effects=True, vmem_limit_bytes=VMEM_LIMIT),
            cost_estimate=pl.CostEstimate(
                flops=2 * matrices * tokens * depth * width,
                bytes_accessed=2 * matrices * (tokens * (depth + width) + depth * width), transcendentals=0),
            name="sums",
        )(a[0], g[0])
        bands = (matrices, 4, depth // 4, width)
        return pl.pallas_call(
            place_kernel,
            out_shape=jax.ShapeDtypeStruct(sums.shape, BF16),
            in_specs=[pl.BlockSpec(memory_space=pl.ANY)],
            out_specs=pl.BlockSpec(memory_space=pl.ANY),
            scratch_shapes=[pltpu.VMEM(bands, BF16), dma(bands[:2]), dma(bands[:2])],
            compiler_params=pltpu.CompilerParams(vmem_limit_bytes=VMEM_LIMIT),
            cost_estimate=pl.CostEstimate(flops=0, bytes_accessed=4 * matrices * depth * width, transcendentals=0),
            name="place",
        )(sums)

    return jax.shard_map(
        step, mesh=mesh,
        in_specs=(P(("rep", "dp"), None, None, None),) * 2,
        out_specs=P("rep", None, None), check_vma=False)
```
